32 devices in a mesh: row: 4 (over y, core), col: 8 (over z, x).
Axes of the slice: x: 2, y: 2, z: 4, core: 2. Of those that a mesh axis runs over, the one named last changes fastest.
Arguments:
- inner_base: bfloat16 [4, 1, 2, 4096, 14336], P(None, None, None, 'row', 'col'), may hold values from -250 to 250
- inner_left: bfloat16 [4, 1, 2, 4096, 16], P(None, None, None, ('row', 'col')), may hold values from -6 to 6
- inner_right: bfloat16 [4, 1, 2, 16, 14336], P(None, None, None, 'row', 'col'), may hold values from -12 to 12
- inner_mag: float32 [4, 1, 2, 14336], P(None, None, None, 'col'), may hold values from 512 to 2048
- outer_base: bfloat16 [4, 1, 14336, 4096], P(None, None, 'row', 'col'), may hold values from -250 to 250
- outer_left: bfloat16 [4, 1, 14336, 16], P(None, None, ('row', 'col')), may hold values from -6 to 6
- outer_right: bfloat16 [4, 1, 16, 4096], P(None, None, 'row', 'col'), may hold values from -12 to 12
- outer_mag: float32 [4, 1, 4096], P(None, None, 'col'), may hold values from 1792 to 7168
Outputs:
- inner_merged: bfloat16 [4, 1, 2, 4096, 14336], P(None, None, None, 'row', 'col')
- outer_merged: bfloat16 [4, 1, 14336, 4096], P(None, None, 'row', 'col')
The draws below stay inside these ranges and needn't reach their ends.
All inputs are finite; a program needn't handle non-finite values.
Results may differ from the reference program's by a relative error of at most 0.001.
Values may be sent and summed in bfloat16 or wider, within the bound.
A program may use at most 256 MiB of HBM per device.

```python
import math
import jax
import jax.numpy as jnp
from jax import lax

D = 4096
FF = 14336
RANK = 16
LAYERS = 4
EXPERTS = 1


def base_draw(key, extent):
    row_count = extent[-2]
    key_one, key_two = jax.random.split(key)
    scale_extent = extent[:-1] + (1,)
    jitter = jnp.clip(jax.random.normal(key_one, extent, jnp.float32), -6.0, 6.0)
    roughness = jnp.exp(jax.random.uniform(key_two, scale_extent, jnp.float32, 0.0, math.log(10.0)))
    growth = 2.0
    position = jnp.arange(row_count, dtype=jnp.float32) / max(row_count - 1, 1)
    rising = 1.0 + growth * position
    return (jitter * roughness * rising[:, None]).astype(jnp.bfloat16)


def draw_inner_base(key, part):
    return base_draw(jax.random.fold_in(key, 11), (LAYERS, EXPERTS, 2, D, FF))


def draw_outer_base(key, part):
    return base_draw(jax.random.fold_in(key, 23), (LAYERS, EXPERTS, FF, D))


def levels(rng, dims, pieces, least, top_value):
    level, own = 1.0, jax.random.fold_in(rng, 6)
    for dim, parts in pieces:
        steps = jnp.exp(jax.random.uniform(jax.random.fold_in(own, dim), (parts,), jnp.float32, least / len(pieces), top_value / len(pieces)))
        level = level * jnp.repeat(steps, dims[dim] // parts).reshape([-1 if axis == dim else 1 for axis in range(len(dims))])
    return level


def gaussian(key, dims, deviation, reach, pieces=(), kind=jnp.bfloat16):
    entries = deviation * jax.random.normal(key, dims, jnp.float32)
    if pieces:
        entries = entries * levels(key, dims, pieces, -0.22, 0.18)
    return jnp.clip(entries, -reach, reach).astype(kind)


def setup_inputs(seed: int = 0) -> dict:
    key_list = jax.random.split(jax.random.key(seed), 9)
    return {
        "inner_base": draw_inner_base(jax.random.fold_in(key_list[8], 71), 0),
        "inner_left": gaussian(key_list[1], (LAYERS, EXPERTS, 2, D, RANK), 1.0, 6.0, ((3, 32),)),
        "inner_right": gaussian(key_list[2], (LAYERS, EXPERTS, 2, RANK, FF), 2.0, 12.0, ((3, 4), (4, 8))),
        "inner_mag": jnp.clip(jnp.exp(math.log(2048.0) - 1.3862944 * jax.random.uniform(key_list[3], (LAYERS, EXPERTS, 2, FF), jnp.float32) ** levels(key_list[3], (LAYERS, EXPERTS, 2, FF), ((3, 8),), -0.2, 0.2)), 512.0, 2048.0),
        "outer_base": draw_outer_base(jax.random.fold_in(key_list[8], 71), 0),
        "outer_left": gaussian(key_list[5], (LAYERS, EXPERTS, FF, RANK), 1.0, 6.0, ((2, 32),)),
        "outer_right": gaussian(key_list[6], (LAYERS, EXPERTS, RANK, D), 2.0, 12.0, ((2, 4), (3, 8))),
        "outer_mag": jnp.clip(jnp.exp(math.log(7168.0) - 1.3862944 * jax.random.uniform(key_list[7], (LAYERS, EXPERTS, D), jnp.float32) ** levels(key_list[7], (LAYERS, EXPERTS, D), ((2, 8),), -0.2, 0.2)), 1792.0, 7168.0),
    }


epsilon = 1e-06

def merge_one(base, left, right, magnitude):
    delta = jnp.einsum('...ik,...kj->...ij', left.astype(jnp.float32), right.astype(jnp.float32))
    combined = base.astype(jnp.float32) + delta
    squares = lax.optimization_barrier(jnp.sum(combined * combined, axis=-2))
    factor = magnitude * lax.rsqrt(squares + epsilon)
    return (factor[..., None, :] * combined).astype(jnp.bfloat16)

def reference(inner_base, inner_left, inner_right, inner_mag, outer_base, outer_left, outer_right, outer_mag):
    inner_layers = []
    outer_layers = []
    for layer_index in range(LAYERS):
        inner_items = []
        outer_items = []
        for expert_index in range(EXPERTS):
            inner_items.append(merge_one(inner_base[layer_index, expert_index], inner_left[layer_index, expert_index], inner_right[layer_index, expert_index], inner_mag[layer_index, expert_index]))
            outer_items.append(merge_one(outer_base[layer_index, expert_index], outer_left[layer_index, expert_index], outer_right[layer_index, expert_index], outer_mag[layer_index, expert_index]))
        inner_layers.append(jnp.stack(inner_items))
        outer_layers.append(jnp.stack(outer_items))
    return (jnp.stack(inner_layers), jnp.stack(outer_layers))
```

```python
import functools

import jax
import jax.numpy as jnp
from jax import lax
from jax.experimental import pallas as pl
from jax.experimental.pallas import tpu as pltpu
from jax.sharding import PartitionSpec as P

epsilon = 1e-06
MESH = pl.DeviceIdType.MESH
ANY = pl.BlockSpec(memory_space=pl.ANY)
VMEM = pl.BlockSpec(memory_space=pltpu.VMEM)
GRANT = 10 << 20
AHEAD = 4
WIDTHS = (256, 128)
HEIGHTS = (512, 896, 256, 128, 64, 32, 16)


def remote(src, dst, send, recv, axis, target):
    return pltpu.make_async_remote_copy(
        src_ref=src, dst_ref=dst, send_sem=send, recv_sem=recv, device_id={axis: target}, device_id_type=MESH
    )


def tiles(rows, cols):
    width = next((w for w in WIDTHS if cols % w == 0), cols)
    height = next(h for h in HEIGHTS if rows % h == 0)
    return height, width


def group_of(count):
    return 2 if count % 2 == 0 else 1


def prepare(left, right, lt, r16, r32, t):
    pieces, _, _, piece = left.shape
    for c in range(pieces):
        lt[t, c * piece : (c + 1) * piece, :] = left[c, t].T
    share = right.shape[2]
    for c in range(right.shape[0]):
        r32[c * share : (c + 1) * share, :] = right[c, t].astype(jnp.float32)
    r16[t] = r32[...].astype(jnp.bfloat16)


def combined(base, lt, r16, t, span, part):
    delta = jnp.dot(lt[t, span, :], r16[t, :, part], preferred_element_type=jnp.float32)
    return base[t, span, part].astype(jnp.float32) + delta


def squares_weight(base, lt, r16, acc, sums, t):
    _, rows, cols = base.shape
    height, width = tiles(rows, cols)
    for j in range(cols // width):
        part = slice(j * width, (j + 1) * width)
        total = jnp.zeros((8, width), jnp.float32)
        for i in range(rows // height):
            full = combined(base, lt, r16, t, slice(i * height, (i + 1) * height), part)
            total = total + jnp.sum((full * full).reshape(height // 8, 8, width), axis=0)
        acc[:, part] = total
    sums[t] = jnp.sum(acc[...], axis=0, keepdims=True)


def scale_weight(base, lt, r16, factor, t):
    _, rows, cols = base.shape
    height, width = tiles(rows, cols)
    for j in range(cols // width):
        part = slice(j * width, (j + 1) * width)
        scale = jnp.broadcast_to(factor[t, :, part], (8, width))
        for i in range(rows // height):
            span = slice(i * height, (i + 1) * height)
            full = combined(base, lt, r16, t, span, part)
            merged = full.reshape(height // 8, 8, width) * scale[None]
            base[t, span, part] = merged.reshape(height, width).astype(jnp.bfloat16)


def collect_kernel(
    rows, cols,
    il, ol, ir, orr, ib, ob, im, om,
    vib, vob, lti, lto, r16i, r16o, fin, fout,
    gil, gol, gir, gor, r32i, r32o, acci, acco, sumi, sumo, heldi, heldo, mi, mo,
    local, loadi, loado, lsi, lri, lso, lro, rsi, rri, rso, rro, xsi, xri, xso, xro,
):
    me_row, me_col = lax.axis_index("row"), lax.axis_index("col")
    row_others = [lax.rem(me_row + k, rows) for k in range(1, rows)]
    row_back = [lax.rem(me_row + rows - k, rows) for k in range(1, rows)]
    col_others = [lax.rem(me_col + k, cols) for k in range(1, cols)]
    col_back = [lax.rem(me_col + cols - k, cols) for k in range(1, cols)]
    barrier = pltpu.get_barrier_semaphore()
    for axis, others in (("row", row_others), ("col", col_others)):
        for other in others:
            pl.semaphore_signal(barrier, inc=1, device_id={axis: other}, device_id_type=MESH)

    own = []
    for number, (src, dst) in enumerate(
        ((ir, gir.at[me_row]), (il, gil.at[me_col]), (orr, gor.at[me_row]), (ol, gol.at[me_col]), (im, mi), (om, mo))
    ):
        copy = pltpu.make_async_copy(src, dst, local.at[number])
        copy.start()
        own.append(copy)

    def load(kind, t):
        src, dst, sem = (ib, vib, loadi) if kind == 0 else (ob, vob, loado)
        return pltpu.make_async_copy(src.at[t], dst.at[t], sem.at[t])

    order = [(0, t) for t in range(ib.shape[0])] + [(1, t) for t in range(ob.shape[0])]
    for item in order[:AHEAD]:
        load(*item).start()
    pl.semaphore_wait(barrier, rows + cols - 2)
    for copy in own:
        copy.wait()

    kinds = (
        (gil, lsi, lri, gir, rsi, rri, xsi, xri, sumi, heldi, mi, fin),
        (gol, lso, lro, gor, rso, rro, xso, xro, sumo, heldo, mo, fout),
    )

    def shares(kind, t):
        left, ls, lr, right, rs, rr = kinds[kind][:6]
        copies = []
        for k, other in enumerate(row_others):
            piece = right.at[me_row, t]
            copies.append(remote(piece, piece, rs.at[t, k], rr.at[t, k], "row", other))
        for k, other in enumerate(col_others):
            piece = left.at[me_col, t]
            copies.append(remote(piece, piece, ls.at[t, k], lr.at[t, k], "col", other))
        return copies

    def arrivals(kind, t):
        left, ls, lr, right, rs, rr = kinds[kind][:6]
        copies = []
        for k, other in enumerate(row_back):
            piece = right.at[other, t]
            copies.append(remote(piece, piece, rs.at[t, k], rr.at[t, k], "row", other))
        for k, other in enumerate(col_back):
            piece = left.at[other, t]
            copies.append(remote(piece, piece, ls.at[t, k], lr.at[t, k], "col", other))
        return copies

    def exchange(kind, t):
        xs, xr, sums, held = kinds[kind][6:10]
        return [
            remote(sums.at[t], held.at[k, t], xs.at[t, k], xr.at[t, k], "row", other)
            for k, other in enumerate(row_others)
        ]

    for kind, count in ((0, ib.shape[0]), (1, ob.shape[0])):

        @pl.loop(0, count)
        def _(t):
            for copy in shares(kind, t):
                copy.start()

    for item in order[AHEAD : AHEAD + 2]:
        load(*item).start()
    waiting = order[AHEAD + 2 :]

    def finish(kind, t):
        xs, xr, sums, held, mag, out = kinds[kind][6:]
        for copy in exchange(kind, t):
            copy.wait_recv()
        total = sums[t]
        for k in range(rows - 1):
            total = total + held[k, t]
        groups = mag.shape[1]
        if groups == 1:
            strength = mag[t]
        else:
            layer, place = lax.div(t, groups), lax.rem(t, groups)
            strength = mag[layer, pl.ds(place, 1), :]
        out[t] = strength * lax.rsqrt(total + epsilon)

    bodies = (
        (vib, lti, r16i, r32i, acci, sumi, gil, gir),
        (vob, lto, r16o, r32o, acco, sumo, gol, gor),
    )
    for kind in (0, 1):
        base, lt, r16, r32, acc, sums, left, right = bodies[kind]
        count = base.shape[0]
        group = group_of(count)
        if kind == 1:
            last = ib.shape[0]
            for t in range(last - group_of(last), last):
                for copy in exchange(0, t):
                    copy.start()

        @pl.loop(0, count // group)
        def _(p):
            first = p * group
            for u in range(group):
                load(kind, first + u).wait()
                for copy in arrivals(kind, first + u):
                    copy.wait_recv()
            done = (0 if kind == 0 else ib.shape[0])
            for u in range(group):
                position = done + first + u
                for number, item in enumerate(waiting):

                    @pl.when(position == number)
                    def _():
                        load(*item).start()

            @pl.when(p > 0)
            def _():
                for u in range(group):
                    for copy in exchange(kind, first - group + u):
                        copy.start()

            for u in range(group):
                prepare(left, right, lt, r16, r32.at[u], first + u)
            for u in range(group):
                squares_weight(base, lt, r16, acc.at[u], sums, first + u)

    count = ob.shape[0]
    early = group_of(ib.shape[0])
    for t in range(early):
        finish(0, t)
    for t in range(count - group_of(count), count):
        for copy in exchange(1, t):
            copy.start()
    for t in range(early):
        scale_weight(vib, lti, r16i, fin, t)

    @pl.loop(early, ib.shape[0])
    def _(t):
        finish(0, t)

    @pl.loop(0, count)
    def _(t):
        finish(1, t)

    for kind, total in ((0, ib.shape[0]), (1, ob.shape[0])):

        @pl.loop(0, total)
        def _(t):
            for copy in shares(kind, t):
                copy.wait_send()
            for copy in exchange(kind, t):
                copy.wait_send()


def scale_kernel(lti, lto, r16i, r16o, fin, fout, ibase, obase, oin, oout, vib, vob, semi, semo):
    early = group_of(vib.shape[0])

    def store(src, dst, sem, t):
        return pltpu.make_async_copy(src.at[t], dst.at[t], sem.at[t])

    for t in range(early):
        store(vib, oin, semi, t).start()
    for base, lt, r16, factor, out, sem, begin in (
        (vib, lti, r16i, fin, oin, semi, early),
        (vob, lto, r16o, fout, oout, semo, 0),
    ):
        count = base.shape[0]
        group = group_of(count)

        @pl.loop(begin // group, count // group)
        def _(p):
            for u in range(group):
                scale_weight(base, lt, r16, factor, p * group + u)
            for u in range(group):
                store(base, out, sem, p * group + u).start()

    for base, out, sem in ((vib, oin, semi), (vob, oout, semo)):

        @pl.loop(0, base.shape[0])
        def _(t):
            store(base, out, sem, t).wait()


def pinned(arrays):
    return [pltpu.with_memory_space_constraint(a, pltpu.VMEM) for a in arrays]


def shards(rows, cols, inner_base, inner_left, inner_right, inner_mag, outer_base, outer_left, outer_right, outer_mag):
    rank = inner_left.shape[-1]
    ib = inner_base.reshape((-1, *inner_base.shape[-2:]))
    ob = outer_base.reshape((-1, *outer_base.shape[-2:]))
    il = jnp.swapaxes(inner_left, -1, -2).reshape((-1, rank, inner_left.shape[-2]))
    ol = jnp.swapaxes(outer_left, -1, -2).reshape((-1, rank, outer_left.shape[-2]))
    ir = inner_right.reshape((-1, *inner_right.shape[-2:]))
    orr = outer_right.reshape((-1, *outer_right.shape[-2:]))
    im = inner_mag.reshape((-1, *inner_mag.shape[-2:]))
    om = outer_mag.reshape((ob.shape[0], 1, -1))
    bf16, f32, dma = jnp.bfloat16, jnp.float32, pltpu.SemaphoreType.DMA
    bases = (ib, ob)
    counts = (ib.shape[0], ob.shape[0])
    scratch = [pltpu.VMEM((n, *a.shape), bf16) for n, a in ((cols, il), (cols, ol), (rows, ir), (rows, orr))]
    scratch += [pltpu.VMEM((group_of(b.shape[0]), rank, b.shape[2]), f32) for b in bases]
    scratch += [pltpu.VMEM((group_of(b.shape[0]), 8, b.shape[2]), f32) for b in bases]
    scratch += [pltpu.VMEM((b.shape[0], 1, b.shape[2]), f32) for b in bases]
    scratch += [pltpu.VMEM((rows - 1, b.shape[0], 1, b.shape[2]), f32) for b in bases]
    scratch += [pltpu.VMEM(m.shape, f32) for m in (im, om)]
    scratch += [dma((6,))] + [dma((n,)) for n in counts]
    for width in (cols - 1, rows - 1, rows - 1):
        for n in counts:
            scratch += [dma((n, width))] * 2
    held = [pltpu.VMEM(b.shape, bf16) for b in bases]
    lefts = [pltpu.VMEM((b.shape[0], b.shape[1], rank), bf16) for b in bases]
    rights = [pltpu.VMEM((b.shape[0], rank, b.shape[2]), bf16) for b in bases]
    factors = [pltpu.VMEM((b.shape[0], 1, b.shape[2]), f32) for b in bases]
    vib, vob, *rest = pinned(
        pl.pallas_call(
            functools.partial(collect_kernel, rows, cols),
            out_shape=held + lefts + rights + factors,
            in_specs=[ANY] * 8,
            out_specs=[VMEM] * 8,
            scratch_shapes=scratch,
            compiler_params=pltpu.CompilerParams(collective_id=0, has_side_effects=True, vmem_limit_bytes=GRANT),
            name="collect",
        )(il, ol, ir, orr, ib, ob, im, om)
    )
    inner, outer, _, _ = pl.pallas_call(
        scale_kernel,
        out_shape=[jax.ShapeDtypeStruct(b.shape, bf16) for b in bases] + held,
        in_specs=[VMEM] * 8,
        out_specs=[ANY] * 2 + [VMEM] * 2,
        input_output_aliases={6: 2, 7: 3},
        scratch_shapes=[dma((n,)) for n in counts],
        compiler_params=pltpu.CompilerParams(vmem_limit_bytes=GRANT),
        name="scale",
    )(*rest, vib, vob)
    return inner.reshape(inner_base.shape), outer.reshape(outer_base.shape)


def solution(mesh):
    in_specs = (
        P(None, None, None, "row", "col"),
        P(None, None, None, ("row", "col"), None),
        P(None, None, None, "row", "col"),
        P(None, None, None, "col"),
        P(None, None, "row", "col"),
        P(None, None, ("row", "col"), None),
        P(None, None, "row", "col"),
        P(None, None, "col"),
    )
    out_specs = (P(None, None, None, "row", "col"), P(None, None, "row", "col"))
    body = functools.partial(shards, mesh.shape["row"], mesh.shape["col"])
    return jax.shard_map(body, mesh=mesh, in_specs=in_specs, out_specs=out_specs, check_vma=False)
```

```python
import functools

import jax
import jax.numpy as jnp
from jax import lax
from jax.experimental import pallas as pl
from jax.experimental.pallas import tpu as pltpu
from jax.sharding import PartitionSpec as P

epsilon = 1e-06
MESH = pl.DeviceIdType.MESH
ANY = pl.BlockSpec(memory_space=pl.ANY)
VMEM = pl.BlockSpec(memory_space=pltpu.VMEM)
GRANT = 10 << 20
AHEAD = 3
WIDTHS = (256, 128)
HEIGHTS = (512, 896, 256, 128, 64, 32, 16)


def remote(src, dst, send, recv, axis, target):
    return pltpu.make_async_remote_copy(
        src_ref=src, dst_ref=dst, send_sem=send, recv_sem=recv, device_id={axis: target}, device_id_type=MESH
    )


def tiles(rows, cols):
    width = next((w for w in WIDTHS if cols % w == 0), cols)
    height = next(h for h in HEIGHTS if rows % h == 0)
    return height, width


def group_of(count):
    return 2 if count % 2 == 0 else 1


def blocks(count, first, size):
    edges = [0, *range(min(first, count), count, size), count]
    return [(begin, end) for begin, end in zip(edges, edges[1:])]


def plans(inner, outer):
    work = [blocks(inner, 2, 3), blocks(outer, 2, 2)]
    return work, [blocks(inner, 2, max(inner, 1)), work[1]]


def peers_of(axis, n):
    me = lax.axis_index(axis)
    low, high, half = lax.rem(me, 2), lax.div(me, 2), n // 2
    partner = me + 1 - 2 * low
    ahead = [lax.rem(high + k, half) * 2 + low for k in range(1, half)]
    behind = [lax.rem(high + half - k, half) * 2 + low for k in range(1, half)]
    return me, partner, ahead, behind


def prepare(left, right, lt, r16, r32, t):
    pieces, _, _, piece = left.shape
    for c in range(pieces):
        lt[t, c * piece : (c + 1) * piece, :] = left[c, t].T
    share = right.shape[2]
    for c in range(right.shape[0]):
        r32[c * share : (c + 1) * share, :] = right[c, t].astype(jnp.float32)
    r16[t] = r32[...].astype(jnp.bfloat16)


def combined(base, lt, r16, t, span, part):
    delta = jnp.dot(lt[t, span, :], r16[t, :, part], preferred_element_type=jnp.float32)
    return base[t, span, part].astype(jnp.float32) + delta


def squares_weight(base, lt, r16, sums, t):
    _, rows, cols = base.shape
    height, width = tiles(rows, cols)
    for j in range(cols // width):
        part = slice(j * width, (j + 1) * width)
        total = jnp.zeros((8, width), jnp.float32)
        for i in range(rows // height):
            full = combined(base, lt, r16, t, slice(i * height, (i + 1) * height), part)
            total = total + jnp.sum((full * full).reshape(height // 8, 8, width), axis=0)
        sums[t, :, part] = jnp.sum(total, axis=0, keepdims=True)


def scale_weight(base, lt, r16, factor, t):
    _, rows, cols = base.shape
    height, width = tiles(rows, cols)
    for j in range(cols // width):
        part = slice(j * width, (j + 1) * width)
        scale = jnp.broadcast_to(factor[t, :, part], (8, width))
        for i in range(rows // height):
            span = slice(i * height, (i + 1) * height)
            full = combined(base, lt, r16, t, span, part)
            merged = full.reshape(height // 8, 8, width) * scale[None]
            base[t, span, part] = merged.reshape(height, width).astype(jnp.bfloat16)


def collect_kernel(
    rows, cols,
    il, ol, ir, orr, ib, ob, im, om,
    vib, vob, lti, lto, r16i, r16o, fin, fout,
    gil, gol, gir, gor, r32i, r32o, sumi, sumo, heldi, heldo, mi, mo,
    local, sent, loadi, loado, nearli, farli, nearlo, farlo, nearri, farri, nearro, farro, xi, xo,
):
    places = {"row": peers_of("row", rows), "col": peers_of("col", cols)}
    me_row, me_col = places["row"][0], places["col"][0]
    row_others = [lax.rem(me_row + k, rows) for k in range(1, rows)]
    barrier = pltpu.get_barrier_semaphore()
    greeted = [("row", other) for other in row_others]
    greeted += [("col", other) for other in [places["col"][1], *places["col"][2]]]
    for axis, other in greeted:
        pl.semaphore_signal(barrier, inc=1, device_id={axis: other}, device_id_type=MESH)

    own = []
    for number, (src, dst) in enumerate(
        ((ir, gir.at[me_row]), (il, gil.at[me_col]), (orr, gor.at[me_row]), (ol, gol.at[me_col]), (im, mi), (om, mo))
    ):
        copy = pltpu.make_async_copy(src, dst, local.at[number])
        copy.start()
        own.append(copy)

    inner, outer = ib.shape[0], ob.shape[0]
    work, cuts = plans(inner, outer)
    flows = (
        {"row": (gir, sent.at[0], nearri, farri), "col": (gil, sent.at[1], nearli, farli)},
        {"row": (gor, sent.at[2], nearro, farro), "col": (gol, sent.at[3], nearlo, farlo)},
    )
    bodies = (
        (ib, vib, loadi, lti, r16i, r32i, gil, gir, sumi, heldi, xi, sent.at[4], mi, fin),
        (ob, vob, loado, lto, r16o, r32o, gol, gor, sumo, heldo, xo, sent.at[5], mo, fout),
    )

    def load(kind, number):
        src, dst, sems = bodies[kind][:3]
        begin, end = work[kind][number]
        span = pl.ds(begin, end - begin)
        whole = pltpu.make_async_copy(src.at[span], dst.at[span], sems.at[number])
        return [pltpu.make_async_copy(src.at[t], dst.at[t], sems.at[number]) for t in range(begin, end)], whole

    def pieces(kind, number, axis, sources, sem):
        data, send, _, _ = flows[kind][axis]
        begin, end = cuts[kind][number]
        place = data.at[sources, pl.ds(begin, end - begin)]
        return remote(place, place, send, sem, axis, places[axis][1])

    def shares(kind, number):
        begin, end = cuts[kind][number]
        for axis in ("row", "col"):
            data, send, near, far = flows[kind][axis]
            me, partner, ahead, _ = places[axis]
            piece = data.at[me, pl.ds(begin, end - begin)]
            for other in ahead:
                remote(piece, piece, send, near.at[number], axis, other).start()
            remote(piece, piece, send, far.at[number], axis, partner).start()

    def forward(kind, number):
        for axis in ("row", "col"):
            _, _, near, far = flows[kind][axis]
            behind = places[axis][3]
            if behind:
                pieces(kind, number, axis, pl.ds(0, len(behind)), near.at[number]).wait_recv()
            for source in behind:
                pieces(kind, number, axis, source, far.at[number]).start()

    def landed(kind, number):
        for axis in ("row", "col"):
            _, _, _, far = flows[kind][axis]
            pieces(kind, number, axis, pl.ds(0, len(places[axis][3]) + 1), far.at[number]).wait_recv()

    def exchange(kind, number):
        sums, held, sems, send = bodies[kind][8:12]
        for t in range(*work[kind][number]):
            for k, other in enumerate(row_others):
                remote(sums.at[t], held.at[k, t], send, sems.at[number], "row", other).start()

    def finish(kind, number):
        sums, held, sems, send, mag, out = bodies[kind][8:]
        begin, end = work[kind][number]
        place = held.at[:, pl.ds(begin, end - begin)]
        remote(place, place, send, sems.at[number], "row", row_others[0]).wait_recv()
        for t in range(begin, end):
            total = sums[t]
            for k in range(rows - 1):
                total = total + held[k, t]
            layer, place = divmod(t, mag.shape[1])
            out[t] = mag[layer, place : place + 1, :] * lax.rsqrt(total + epsilon)

    pl.semaphore_wait(barrier, len(greeted))
    for copy in own:
        copy.wait()
    for kind in (0, 1):
        for number in range(len(cuts[kind])):
            shares(kind, number)
    order = [(kind, number) for kind in (0, 1) for number in range(len(work[kind]))]
    for item in order[:AHEAD]:
        for copy in load(*item)[0]:
            copy.start(priority=1)
    for number in range(len(cuts[0])):
        forward(0, number)

    for place, (kind, number) in enumerate(order):
        begin, end = work[kind][number]
        load(kind, number)[1].wait()
        for group, cut in enumerate(cuts[kind]):
            if cut[0] == begin:
                landed(kind, group)
        for group in range(len(cuts[1])):
            if place == min(1 + group, len(work[0]) - 1):
                forward(1, group)
        if place + AHEAD < len(order):
            for copy in load(*order[place + AHEAD])[0]:
                copy.start(priority=1)
        if place > 0:
            exchange(*order[place - 1])
        if place > 1:
            finish(*order[place - 2])
        _, base, _, lt, r16, r32, left, right, sums = bodies[kind][:9]
        for t in range(begin, end):
            prepare(left, right, lt, r16, r32.at[t - begin], t)
            squares_weight(base, lt, r16, sums, t)

    if len(order) > 1:
        finish(*order[-2])
    exchange(*order[-1])
    for t in range(work[0][0][1]):
        scale_weight(vib, lti, r16i, fin, t)
    finish(*order[-1])

    for kind in (0, 1):
        for axis in ("row", "col"):
            data, send, near, _ = flows[kind][axis]
            place = data.at[pl.ds(0, data.shape[0] - 1)]
            remote(place, place, send, near.at[0], axis, places[axis][1]).wait_send()
        held, sems, send = bodies[kind][9:12]
        remote(held, held, send, sems.at[0], "row", row_others[0]).wait_send()


def scale_kernel(lti, lto, r16i, r16o, fin, fout, ibase, obase, oin, oout, vib, vob, sems):
    early = plans(vib.shape[0], vob.shape[0])[0][0][0][1]
    for t in range(early):
        pltpu.make_async_copy(vib.at[t], oin.at[t], sems.at[0]).start()
    for number, (base, lt, r16, factor, out, begin) in enumerate(
        ((vib, lti, r16i, fin, oin, early), (vob, lto, r16o, fout, oout, 0))
    ):
        group = group_of(base.shape[0] - begin)

        @pl.loop(0, (base.shape[0] - begin) // group)
        def _(p):
            first = begin + p * group
            for u in range(group):
                scale_weight(base, lt, r16, factor, first + u)
            for u in range(group):
                pltpu.make_async_copy(base.at[first + u], out.at[first + u], sems.at[number]).start()

    pltpu.make_async_copy(vib, oin, sems.at[0]).wait()
    pltpu.make_async_copy(vob, oout, sems.at[1]).wait()


def pinned(arrays):
    return [pltpu.with_memory_space_constraint(a, pltpu.VMEM) for a in arrays]


def shards(rows, cols, inner_base, inner_left, inner_right, inner_mag, outer_base, outer_left, outer_right, outer_mag):
    rank = inner_left.shape[-1]
    ib = inner_base.reshape((-1, *inner_base.shape[-2:]))
    ob = outer_base.reshape((-1, *outer_base.shape[-2:]))
    il = jnp.swapaxes(inner_left, -1, -2).reshape((-1, rank, inner_left.shape[-2]))
    ol = jnp.swapaxes(outer_left, -1, -2).reshape((-1, rank, outer_left.shape[-2]))
    ir = inner_right.reshape((-1, *inner_right.shape[-2:]))
    orr = outer_right.reshape((-1, *outer_right.shape[-2:]))
    im = inner_mag.reshape((-1, *inner_mag.shape[-2:]))
    om = outer_mag.reshape((ob.shape[0], 1, -1))
    bf16, f32, dma = jnp.bfloat16, jnp.float32, pltpu.SemaphoreType.DMA
    bases = (ib, ob)
    work, cuts = plans(ib.shape[0], ob.shape[0])
    scratch = [pltpu.VMEM((n, *a.shape), bf16) for n, a in ((cols, il), (cols, ol), (rows, ir), (rows, orr))]
    for b, edges in zip(bases, work):
        scratch.append(pltpu.VMEM((max(end - begin for begin, end in edges), rank, b.shape[2]), f32))
    scratch += [pltpu.VMEM((b.shape[0], 1, b.shape[2]), f32) for b in bases]
    scratch += [pltpu.VMEM((rows - 1, b.shape[0], 1, b.shape[2]), f32) for b in bases]
    scratch += [pltpu.VMEM(m.shape, f32) for m in (im, om)]
    scratch += [dma((6,)), dma((6,))] + [dma((len(edges),)) for edges in work]
    for _ in range(2):
        for edges in cuts:
            scratch += [dma((len(edges),))] * 2
    scratch += [dma((len(edges),)) for edges in work]
    held = [pltpu.VMEM(b.shape, bf16) for b in bases]
    lefts = [pltpu.VMEM((b.shape[0], b.shape[1], rank), bf16) for b in bases]
    rights = [pltpu.VMEM((b.shape[0], rank, b.shape[2]), bf16) for b in bases]
    factors = [pltpu.VMEM((b.shape[0], 1, b.shape[2]), f32) for b in bases]
    vib, vob, *rest = pinned(
        pl.pallas_call(
            functools.partial(collect_kernel, rows, cols),
            out_shape=held + lefts + rights + factors,
            in_specs=[ANY] * 8,
            out_specs=[VMEM] * 8,
            scratch_shapes=scratch,
            compiler_params=pltpu.CompilerParams(collective_id=0, has_side_effects=True, vmem_limit_bytes=GRANT),
            name="collect",
        )(il, ol, ir, orr, ib, ob, im, om)
    )
    inner, outer, _, _ = pl.pallas_call(
        scale_kernel,
        out_shape=[jax.ShapeDtypeStruct(b.shape, bf16) for b in bases] + held,
        in_specs=[VMEM] * 8,
        out_specs=[ANY] * 2 + [VMEM] * 2,
        input_output_aliases={6: 2, 7: 3},
        scratch_shapes=[dma((2,))],
        compiler_params=pltpu.CompilerParams(vmem_limit_bytes=GRANT),
        name="scale",
    )(*rest, vib, vob)
    return inner.reshape(inner_base.shape), outer.reshape(outer_base.shape)


def solution(mesh):
    in_specs = (
        P(None, None, None, "row", "col"),
        P(None, None, None, ("row", "col"), None),
        P(None, None, None, "row", "col"),
        P(None, None, None, "col"),
        P(None, None, "row", "col"),
        P(None, None, ("row", "col"), None),
        P(None, None, "row", "col"),
        P(None, None, "col"),
    )
    out_specs = (P(None, None, None, "row", "col"), P(None, None, "row", "col"))
    body = functools.partial(shards, mesh.shape["row"], mesh.shape["col"])
    return jax.shard_map(body, mesh=mesh, in_specs=in_specs, out_specs=out_specs, check_vma=False)
```

```python
import functools

import jax
import jax.numpy as jnp
from jax import lax
from jax.experimental import pallas as pl
from jax.experimental.pallas import tpu as pltpu
from jax.sharding import PartitionSpec as P

epsilon = 1e-06
MESH = pl.DeviceIdType.MESH
ANY = pl.BlockSpec(memory_space=pl.ANY)
VMEM = pl.BlockSpec(memory_space=pltpu.VMEM)
GRANT = 10 << 20
AHEAD = 3
WIDTHS = (256, 128)


def remote(src, dst, send, recv, axis, target):
    return pltpu.make_async_remote_copy(
        src_ref=src, dst_ref=dst, send_sem=send, recv_sem=recv, device_id={axis: target}, device_id_type=MESH
    )


def width_of(cols):
    return next((w for w in WIDTHS if cols % w == 0), cols)


def group_of(count):
    return 2 if count % 2 == 0 else 1


def blocks(count, first, size):
    edges = [0, *range(min(first, count), count, size), count]
    return [(begin, end) for begin, end in zip(edges, edges[1:])]


def plans(inner, outer):
    work = [blocks(inner, 2, 3), blocks(outer, 2, 2)]
    return work, [blocks(inner, 2, max(inner, 1)), work[1]]


def peers_of(axis, n):
    me = lax.axis_index(axis)
    low, high, half = lax.rem(me, 2), lax.div(me, 2), n // 2
    partner = me + 1 - 2 * low
    ahead = [lax.rem(high + k, half) * 2 + low for k in range(1, half)]
    behind = [lax.rem(high + half - k, half) * 2 + low for k in range(1, half)]
    return me, partner, ahead, behind


def sources_of(cols):
    me, partner, _, behind = peers_of("col", cols)
    return [me, *behind, partner, *(source + partner - me for source in behind)]


def slots_of(cols):
    me, half = lax.axis_index("col"), cols // 2
    low, high = lax.rem(me, 2), lax.div(me, 2)
    return [lax.rem(high + half - c // 2, half) + half * lax.rem(low + c, 2) for c in range(cols)]


def prepare_left(left, lt, t, sources, slots):
    for k in slots:
        lt[t, k] = left[sources[k], t].T


def prepare_right(right, r16, r32, t):
    share = right.shape[2]
    for c in range(right.shape[0]):
        r32[c * share : (c + 1) * share, :] = right[c, t].astype(jnp.float32)
    r16[t] = r32[...].astype(jnp.bfloat16)


def combined(base, lt, r16, t, span, slot, part):
    delta = jnp.dot(lt[t, slot], r16[t, :, part], preferred_element_type=jnp.float32)
    return base[t, span, part].astype(jnp.float32) + delta


def squares_weight(base, lt, r16, t, sources, slots, totals, save):
    piece, cols = lt.shape[2], base.shape[2]
    width = width_of(cols)
    for j in range(cols // width):
        part = slice(j * width, (j + 1) * width)
        total = jnp.zeros((8, width), jnp.float32) if totals is None else totals[:, part]
        for k in slots:
            span = pl.ds(pl.multiple_of(sources[k] * piece, piece), piece)
            full = combined(base, lt, r16, t, span, k, part)
            total = total + jnp.sum((full * full).reshape(piece // 8, 8, width), axis=0)
        save(part, total)


def scale_weight(base, lt, r16, factor, t, slots):
    piece, cols = lt.shape[2], base.shape[2]
    width = width_of(cols)
    for j in range(cols // width):
        part = slice(j * width, (j + 1) * width)
        scale = jnp.broadcast_to(factor[t, :, part], (8, width))
        for c, slot in enumerate(slots):
            span = slice(c * piece, (c + 1) * piece)
            full = combined(base, lt, r16, t, span, slot, part)
            merged = full.reshape(piece // 8, 8, width) * scale[None]
            base[t, span, part] = merged.reshape(piece, width).astype(jnp.bfloat16)


def collect_kernel(
    rows, cols,
    il, ol, ir, orr, ib, ob, im, om,
    vib, vob, lti, lto, r16i, r16o, fin, fout,
    gil, gol, gir, gor, r32i, r32o, acc, sumi, sumo, heldi, heldo, mi, mo,
    local, sent, loadi, loado, nearli, farli, nearlo, farlo, nearri, farri, nearro, farro, xi, xo,
):
    places = {"row": peers_of("row", rows), "col": peers_of("col", cols)}
    me_row, me_col = places["row"][0], places["col"][0]
    row_others = [lax.rem(me_row + k, rows) for k in range(1, rows)]
    barrier = pltpu.get_barrier_semaphore()
    greeted = [("row", other) for other in row_others]
    greeted += [("col", other) for other in [places["col"][1], *places["col"][2]]]
    for axis, other in greeted:
        pl.semaphore_signal(barrier, inc=1, device_id={axis: other}, device_id_type=MESH)

    own = []
    for number, (src, dst) in enumerate(
        ((ir, gir.at[me_row]), (il, gil.at[me_col]), (orr, gor.at[me_row]), (ol, gol.at[me_col]), (im, mi), (om, mo))
    ):
        copy = pltpu.make_async_copy(src, dst, local.at[number])
        copy.start()
        own.append(copy)

    inner, outer = ib.shape[0], ob.shape[0]
    work, cuts = plans(inner, outer)
    flows = (
        {"row": (gir, sent.at[0], nearri, farri), "col": (gil, sent.at[1], nearli, farli)},
        {"row": (gor, sent.at[2], nearro, farro), "col": (gol, sent.at[3], nearlo, farlo)},
    )
    bodies = (
        (ib, vib, loadi, lti, r16i, r32i, gil, gir, sumi, heldi, xi, sent.at[4], mi, fin),
        (ob, vob, loado, lto, r16o, r32o, gol, gor, sumo, heldo, xo, sent.at[5], mo, fout),
    )

    def load(kind, number):
        src, dst, sems = bodies[kind][:3]
        begin, end = work[kind][number]
        span = pl.ds(begin, end - begin)
        whole = pltpu.make_async_copy(src.at[span], dst.at[span], sems.at[number])
        return [pltpu.make_async_copy(src.at[t], dst.at[t], sems.at[number]) for t in range(begin, end)], whole

    def pieces(kind, number, axis, sources, sem):
        data, send, _, _ = flows[kind][axis]
        begin, end = cuts[kind][number]
        place = data.at[sources, pl.ds(begin, end - begin)]
        return remote(place, place, send, sem, axis, places[axis][1])

    def shares(kind, number):
        begin, end = cuts[kind][number]
        for axis in ("col", "row"):
            data, send, near, far = flows[kind][axis]
            me, partner, ahead, _ = places[axis]
            piece = data.at[me, pl.ds(begin, end - begin)]
            for other in ahead:
                remote(piece, piece, send, near.at[number], axis, other).start()
            arrival = near if axis == "col" else far
            remote(piece, piece, send, arrival.at[number], axis, partner).start()

    def forward(kind, number):
        for axis in ("col", "row"):
            _, _, near, far = flows[kind][axis]
            behind = places[axis][3]
            direct = len(behind) + (1 if axis == "col" else 0)
            if direct:
                pieces(kind, number, axis, pl.ds(0, direct), near.at[number]).wait_recv()
            for source in behind:
                pieces(kind, number, axis, source, far.at[number]).start()

    def landed(kind, number, axis):
        _, _, _, far = flows[kind][axis]
        relayed = len(places[axis][3]) + (0 if axis == "col" else 1)
        if relayed:
            pieces(kind, number, axis, pl.ds(0, relayed), far.at[number]).wait_recv()

    def exchange(kind, number):
        sums, held, sems, send = bodies[kind][8:12]
        for t in range(*work[kind][number]):
            for k, other in enumerate(row_others):
                remote(sums.at[t], held.at[k, t], send, sems.at[number], "row", other).start()

    def finish(kind, number):
        sums, held, sems, send, mag, out = bodies[kind][8:]
        begin, end = work[kind][number]
        place = held.at[:, pl.ds(begin, end - begin)]
        remote(place, place, send, sems.at[number], "row", row_others[0]).wait_recv()
        for t in range(begin, end):
            total = sums[t]
            for k in range(rows - 1):
                total = total + held[k, t]
            layer, place = divmod(t, mag.shape[1])
            out[t] = mag[layer, place : place + 1, :] * lax.rsqrt(total + epsilon)

    pl.semaphore_wait(barrier, len(greeted))
    for copy in own:
        copy.wait()
    for kind in (0, 1):
        for number in range(len(cuts[kind])):
            shares(kind, number)
    order = [(kind, number) for kind in (0, 1) for number in range(len(work[kind]))]
    for item in order[:AHEAD]:
        for copy in load(*item)[0]:
            copy.start(priority=1)
    forward(0, 0)
    sources = sources_of(cols)
    direct, relayed = range(cols // 2 + 1), range(cols // 2 + 1, cols)
    ready = set()
    pending = [(0, number) for number in range(1, len(cuts[0]))] + [(1, number) for number in range(len(cuts[1]))]

    for place, (kind, number) in enumerate(order):
        begin, end = work[kind][number]
        _, base, _, lt, r16, r32, left, right, sums = bodies[kind][:9]
        split = kind == 0 and place < len(cuts[0])
        load(kind, number)[1].wait()
        while pending and not split:
            forward(*pending.pop(0))
        arrived = [group for group, cut in enumerate(cuts[kind]) if cut[0] == begin]
        for group in arrived:
            landed(kind, group, "row")
            if not split:
                landed(kind, group, "col")
        if place + AHEAD < len(order):
            for copy in load(*order[place + AHEAD])[0]:
                copy.start(priority=1)
        if place > 0:
            exchange(*order[place - 1])
        if place > 1:
            finish(*order[place - 2])
        ahead = order[place + 1] if place + 1 < len(order) and order[place + 1][0] == 1 and not pending else None

        def whole(t):
            def save(part, total):
                sums[t, :, part] = jnp.sum(total, axis=0, keepdims=True)

            return save

        def partial(u):
            def save(part, total):
                acc[u, :, part] = total

            return save

        for t in range(begin, end):
            prepare_right(right, r16, r32.at[t - begin], t)
            if split:
                prepare_left(left, lt, t, sources, direct)
                squares_weight(base, lt, r16, t, sources, direct, None, partial(t - begin))
                continue
            prepare_left(left, lt, t, sources, relayed if (kind, t) in ready else range(cols))
            if t == begin and ahead is not None:
                for later in range(*work[1][ahead[1]]):
                    prepare_left(gol, lto, later, sources, direct)
                    ready.add((1, later))
            squares_weight(base, lt, r16, t, sources, range(cols), None, whole(t))
        if not split:
            continue
        if pending:
            forward(*pending.pop(0))
        for group in arrived:
            landed(kind, group, "col")
        for t in range(begin, end):
            prepare_left(left, lt, t, sources, relayed)
            squares_weight(base, lt, r16, t, sources, relayed, acc.at[t - begin], whole(t))

    if len(order) > 1:
        finish(*order[-2])
    exchange(*order[-1])
    for t in range(work[0][0][1]):
        scale_weight(vib, lti, r16i, fin, t, slots_of(cols))
    finish(*order[-1])

    for kind in (0, 1):
        for axis in ("row", "col"):
            data, send, near, _ = flows[kind][axis]
            place = data.at[pl.ds(0, data.shape[0] - 1)]
            remote(place, place, send, near.at[0], axis, places[axis][1]).wait_send()
        held, sems, send = bodies[kind][9:12]
        remote(held, held, send, sems.at[0], "row", row_others[0]).wait_send()


def scale_kernel(cols, lti, lto, r16i, r16o, fin, fout, ibase, obase, oin, oout, vib, vob, sems):
    slots = slots_of(cols)
    early = plans(vib.shape[0], vob.shape[0])[0][0][0][1]
    for t in range(early):
        pltpu.make_async_copy(vib.at[t], oin.at[t], sems.at[0]).start()
    for number, (base, lt, r16, factor, out, begin) in enumerate(
        ((vib, lti, r16i, fin, oin, early), (vob, lto, r16o, fout, oout, 0))
    ):
        group = group_of(base.shape[0] - begin)

        @pl.loop(0, (base.shape[0] - begin) // group)
        def _(p):
            first = begin + p * group
            for u in range(group):
                scale_weight(base, lt, r16, factor, first + u, slots)
            for u in range(group):
                pltpu.make_async_copy(base.at[first + u], out.at[first + u], sems.at[number]).start()

    pltpu.make_async_copy(vib, oin, sems.at[0]).wait()
    pltpu.make_async_copy(vob, oout, sems.at[1]).wait()


def pinned(arrays):
    return [pltpu.with_memory_space_constraint(a, pltpu.VMEM) for a in arrays]


def shards(rows, cols, inner_base, inner_left, inner_right, inner_mag, outer_base, outer_left, outer_right, outer_mag):
    rank = inner_left.shape[-1]
    ib = inner_base.reshape((-1, *inner_base.shape[-2:]))
    ob = outer_base.reshape((-1, *outer_base.shape[-2:]))
    il = jnp.swapaxes(inner_left, -1, -2).reshape((-1, rank, inner_left.shape[-2]))
    ol = jnp.swapaxes(outer_left, -1, -2).reshape((-1, rank, outer_left.shape[-2]))
    ir = inner_right.reshape((-1, *inner_right.shape[-2:]))
    orr = outer_right.reshape((-1, *outer_right.shape[-2:]))
    im = inner_mag.reshape((-1, *inner_mag.shape[-2:]))
    om = outer_mag.reshape((ob.shape[0], 1, -1))
    bf16, f32, dma = jnp.bfloat16, jnp.float32, pltpu.SemaphoreType.DMA
    bases = (ib, ob)
    work, cuts = plans(ib.shape[0], ob.shape[0])
    scratch = [pltpu.VMEM((n, *a.shape), bf16) for n, a in ((cols, il), (cols, ol), (rows, ir), (rows, orr))]
    for b, edges in zip(bases, work):
        scratch.append(pltpu.VMEM((max(end - begin for begin, end in edges), rank, b.shape[2]), f32))
    scratch.append(pltpu.VMEM((max(end - begin for begin, end in work[0]), 8, ib.shape[2]), f32))
    scratch += [pltpu.VMEM((b.shape[0], 1, b.shape[2]), f32) for b in bases]
    scratch += [pltpu.VMEM((rows - 1, b.shape[0], 1, b.shape[2]), f32) for b in bases]
    scratch += [pltpu.VMEM(m.shape, f32) for m in (im, om)]
    scratch += [dma((6,)), dma((6,))] + [dma((len(edges),)) for edges in work]
    for _ in range(2):
        for edges in cuts:
            scratch += [dma((len(edges),))] * 2
    scratch += [dma((len(edges),)) for edges in work]
    held = [pltpu.VMEM(b.shape, bf16) for b in bases]
    lefts = [pltpu.VMEM((b.shape[0], cols, b.shape[1] // cols, rank), bf16) for b in bases]
    rights = [pltpu.VMEM((b.shape[0], rank, b.shape[2]), bf16) for b in bases]
    factors = [pltpu.VMEM((b.shape[0], 1, b.shape[2]), f32) for b in bases]
    vib, vob, *rest = pinned(
        pl.pallas_call(
            functools.partial(collect_kernel, rows, cols),
            out_shape=held + lefts + rights + factors,
            in_specs=[ANY] * 8,
            out_specs=[VMEM] * 8,
            scratch_shapes=scratch,
            compiler_params=pltpu.CompilerParams(collective_id=0, has_side_effects=True, vmem_limit_bytes=GRANT),
            name="collect",
        )(il, ol, ir, orr, ib, ob, im, om)
    )
    inner, outer, _, _ = pl.pallas_call(
        functools.partial(scale_kernel, cols),
        out_shape=[jax.ShapeDtypeStruct(b.shape, bf16) for b in bases] + held,
        in_specs=[VMEM] * 8,
        out_specs=[ANY] * 2 + [VMEM] * 2,
        input_output_aliases={6: 2, 7: 3},
        scratch_shapes=[dma((2,))],
        compiler_params=pltpu.CompilerParams(vmem_limit_bytes=GRANT),
        name="scale",
    )(*rest, vib, vob)
    return inner.reshape(inner_base.shape), outer.reshape(outer_base.shape)


def solution(mesh):
    in_specs = (
        P(None, None, None, "row", "col"),
        P(None, None, None, ("row", "col"), None),
        P(None, None, None, "row", "col"),
        P(None, None, None, "col"),
        P(None, None, "row", "col"),
        P(None, None, ("row", "col"), None),
        P(None, None, "row", "col"),
        P(None, None, "col"),
    )
    out_specs = (P(None, None, None, "row", "col"), P(None, None, "row", "col"))
    body = functools.partial(shards, mesh.shape["row"], mesh.shape["col"])
    return jax.shard_map(body, mesh=mesh, in_specs=in_specs, out_specs=out_specs, check_vma=False)
```

```python
import functools

import jax
import jax.numpy as jnp
from jax import lax
from jax.experimental import pallas as pl
from jax.experimental.pallas import tpu as pltpu
from jax.sharding import PartitionSpec as P

epsilon = 1e-06
MESH = pl.DeviceIdType.MESH
ANY = pl.BlockSpec(memory_space=pl.ANY)
VMEM = pl.BlockSpec(memory_space=pltpu.VMEM)
GRANT = 10 << 20
AHEAD = 3
WIDTHS = (256, 128)


def remote(src, dst, send, recv, axis, target):
    return pltpu.make_async_remote_copy(
        src_ref=src, dst_ref=dst, send_sem=send, recv_sem=recv, device_id={axis: target}, device_id_type=MESH
    )


def width_of(cols):
    return next((w for w in WIDTHS if cols % w == 0), cols)


def group_of(count):
    return 2 if count % 2 == 0 else 1


def blocks(count, first, size):
    edges = [0, *range(min(first, count), count, size), count]
    return [(begin, end) for begin, end in zip(edges, edges[1:])]


def plans(inner, outer):
    work = [blocks(inner, 2, 3), blocks(outer, 2, 2)]
    return work, [blocks(inner, 2, max(inner, 1)), work[1]]


def peers_of(axis, n):
    me = lax.axis_index(axis)
    low, high, half = lax.rem(me, 2), lax.div(me, 2), n // 2
    partner = me + 1 - 2 * low
    ahead = [lax.rem(high + k, half) * 2 + low for k in range(1, half)]
    behind = [lax.rem(high + half - k, half) * 2 + low for k in range(1, half)]
    return me, partner, ahead, behind


def sources_of(cols):
    me, partner, _, behind = peers_of("col", cols)
    return [me, *behind, partner, *(source + partner - me for source in behind)]


def slots_of(cols):
    me, half = lax.axis_index("col"), cols // 2
    low, high = lax.rem(me, 2), lax.div(me, 2)
    return [lax.rem(high + half - c // 2, half) + half * lax.rem(low + c, 2) for c in range(cols)]


def prepare_left(left, lt, t, sources, slots):
    for k in slots:
        lt[t, k] = left[sources[k], t].T


def prepare_right(right, r16, r32, t):
    share = right.shape[2]
    for c in range(right.shape[0]):
        r32[c * share : (c + 1) * share, :] = right[c, t].astype(jnp.float32)
    r16[t] = r32[...].astype(jnp.bfloat16)


def combined(base, lt, r16, t, span, slot, part):
    delta = jnp.dot(lt[t, slot], r16[t, :, part], preferred_element_type=jnp.float32)
    return base[t, span, part].astype(jnp.float32) + delta


def squares_weight(base, lt, r16, t, sources, slots, totals, save):
    piece, cols = lt.shape[2], base.shape[2]
    width = width_of(cols)
    for j in range(cols // width):
        part = slice(j * width, (j + 1) * width)
        total = jnp.zeros((8, width), jnp.float32) if totals is None else totals[:, part]
        for k in slots:
            span = pl.ds(pl.multiple_of(sources[k] * piece, piece), piece)
            full = combined(base, lt, r16, t, span, k, part)
            total = total + jnp.sum((full * full).reshape(piece // 8, 8, width), axis=0)
        save(part, total)


def scale_weight(base, lt, r16, factor, t, slots):
    piece, cols = lt.shape[2], base.shape[2]
    width = width_of(cols)
    for j in range(cols // width):
        part = slice(j * width, (j + 1) * width)
        scale = jnp.broadcast_to(factor[t, :, part], (8, width))
        for c, slot in enumerate(slots):
            span = slice(c * piece, (c + 1) * piece)
            full = combined(base, lt, r16, t, span, slot, part)
            merged = full.reshape(piece // 8, 8, width) * scale[None]
            base[t, span, part] = merged.reshape(piece, width).astype(jnp.bfloat16)


def collect_kernel(
    rows, cols,
    il, ol, ir, orr, ib, ob, im, om,
    vib, vob, lti, lto, r16i, r16o, fin, fout,
    gil, gol, gir, gor, r32i, r32o, acc, sumi, sumo, heldi, heldo, mi, mo,
    local, sent, loadi, loado, nearli, farli, nearlo, farlo, nearri, farri, nearro, farro, xi, xo,
):
    places = {"row": peers_of("row", rows), "col": peers_of("col", cols)}
    me_row, me_col = places["row"][0], places["col"][0]
    row_others = [lax.rem(me_row + k, rows) for k in range(1, rows)]
    barrier = pltpu.get_barrier_semaphore()
    greeted = [("row", other) for other in row_others]
    greeted += [("col", other) for other in [places["col"][1], *places["col"][2]]]
    for axis, other in greeted:
        pl.semaphore_signal(barrier, inc=1, device_id={axis: other}, device_id_type=MESH)

    own = []
    for number, (src, dst) in enumerate(
        ((ir, gir.at[me_row]), (il, gil.at[me_col]), (orr, gor.at[me_row]), (ol, gol.at[me_col]), (im, mi), (om, mo))
    ):
        copy = pltpu.make_async_copy(src, dst, local.at[number])
        copy.start()
        own.append(copy)

    inner, outer = ib.shape[0], ob.shape[0]
    work, cuts = plans(inner, outer)
    flows = (
        {"row": (gir, sent.at[0], nearri, farri), "col": (gil, sent.at[1], nearli, farli)},
        {"row": (gor, sent.at[2], nearro, farro), "col": (gol, sent.at[3], nearlo, farlo)},
    )
    bodies = (
        (ib, vib, loadi, lti, r16i, r32i, gil, gir, sumi, heldi, xi, sent.at[4], mi, fin),
        (ob, vob, loado, lto, r16o, r32o, gol, gor, sumo, heldo, xo, sent.at[5], mo, fout),
    )

    def load(kind, number):
        src, dst, sems = bodies[kind][:3]
        begin, end = work[kind][number]
        span = pl.ds(begin, end - begin)
        whole = pltpu.make_async_copy(src.at[span], dst.at[span], sems.at[number])
        return [pltpu.make_async_copy(src.at[t], dst.at[t], sems.at[number]) for t in range(begin, end)], whole

    def pieces(kind, number, axis, sources, sem):
        data, send, _, _ = flows[kind][axis]
        begin, end = cuts[kind][number]
        place = data.at[sources, pl.ds(begin, end - begin)]
        return remote(place, place, send, sem, axis, places[axis][1])

    def shares(kind, number):
        begin, end = cuts[kind][number]
        for axis in ("col", "row"):
            data, send, near, far = flows[kind][axis]
            me, partner, ahead, _ = places[axis]
            piece = data.at[me, pl.ds(begin, end - begin)]
            for other in ahead:
                remote(piece, piece, send, near.at[number], axis, other).start()
            arrival = near if axis == "col" else far
            remote(piece, piece, send, arrival.at[number], axis, partner).start()

    def forward(kind, number):
        for axis in ("col", "row"):
            _, _, near, far = flows[kind][axis]
            behind = places[axis][3]
            direct = len(behind) + (1 if axis == "col" else 0)
            if direct:
                pieces(kind, number, axis, pl.ds(0, direct), near.at[number]).wait_recv()
            for source in behind:
                pieces(kind, number, axis, source, far.at[number]).start()

    def landed(kind, number, axis):
        _, _, _, far = flows[kind][axis]
        relayed = len(places[axis][3]) + (0 if axis == "col" else 1)
        if relayed:
            pieces(kind, number, axis, pl.ds(0, relayed), far.at[number]).wait_recv()

    def exchange(kind, number):
        sums, held, sems, send = bodies[kind][8:12]
        for t in range(*work[kind][number]):
            for k, other in enumerate(row_others):
                remote(sums.at[t], held.at[k, t], send, sems.at[number], "row", other).start()

    def finish(kind, number):
        sums, held, sems, send, mag, out = bodies[kind][8:]
        begin, end = work[kind][number]
        place = held.at[:, pl.ds(begin, end - begin)]
        remote(place, place, send, sems.at[number], "row", row_others[0]).wait_recv()
        for t in range(begin, end):
            total = sums[t]
            for k in range(rows - 1):
                total = total + held[k, t]
            layer, place = divmod(t, mag.shape[1])
            out[t] = mag[layer, place : place + 1, :] * lax.rsqrt(total + epsilon)

    pl.semaphore_wait(barrier, len(greeted))
    for copy in own:
        copy.wait()
    for kind in (0, 1):
        for number in range(len(cuts[kind])):
            shares(kind, number)
    order = [(kind, number) for kind in (0, 1) for number in range(len(work[kind]))]
    for item in order[:AHEAD]:
        for copy in load(*item)[0]:
            copy.start(priority=1)
    forward(0, 0)
    sources = sources_of(cols)
    direct, relayed = range(cols // 2 + 1), range(cols // 2 + 1, cols)
    ready = set()
    pending = [(0, number) for number in range(1, len(cuts[0]))] + [(1, number) for number in range(len(cuts[1]))]

    for place, (kind, number) in enumerate(order):
        begin, end = work[kind][number]
        _, base, _, lt, r16, r32, left, right, sums = bodies[kind][:9]
        split = kind == 0 and place < len(cuts[0])
        load(kind, number)[1].wait()
        while pending and not split:
            forward(*pending.pop(0))
        arrived = [group for group, cut in enumerate(cuts[kind]) if cut[0] == begin]
        for group in arrived:
            landed(kind, group, "row")
            if not split:
                landed(kind, group, "col")
        if place + AHEAD < len(order):
            for copy in load(*order[place + AHEAD])[0]:
                copy.start(priority=1)
        if place > 0:
            exchange(*order[place - 1])
        if place > 2:
            finish(*order[place - 3])
        ahead = order[place + 1] if place + 1 < len(order) and order[place + 1][0] == 1 and not pending else None

        def whole(t):
            def save(part, total):
                sums[t, :, part] = jnp.sum(total, axis=0, keepdims=True)

            return save

        def partial(u):
            def save(part, total):
                acc[u, :, part] = total

            return save

        for t in range(begin, end):
            prepare_right(right, r16, r32.at[t - begin], t)
            if split:
                prepare_left(left, lt, t, sources, direct)
                squares_weight(base, lt, r16, t, sources, direct, None, partial(t - begin))
                continue
            prepare_left(left, lt, t, sources, relayed if (kind, t) in ready else range(cols))
            if t == begin and ahead is not None:
                for later in range(*work[1][ahead[1]]):
                    prepare_left(gol, lto, later, sources, direct)
                    ready.add((1, later))
            squares_weight(base, lt, r16, t, sources, range(cols), None, whole(t))
        if not split:
            continue
        if pending:
            forward(*pending.pop(0))
        for group in arrived:
            landed(kind, group, "col")
        for t in range(begin, end):
            prepare_left(left, lt, t, sources, relayed)
            squares_weight(base, lt, r16, t, sources, relayed, acc.at[t - begin], whole(t))

    if len(order) > 2:
        finish(*order[-3])
    exchange(*order[-1])
    if len(order) > 1:
        finish(*order[-2])
    for t in range(work[0][0][1]):
        scale_weight(vib, lti, r16i, fin, t, slots_of(cols))
    finish(*order[-1])

    for kind in (0, 1):
        for axis in ("row", "col"):
            data, send, near, _ = flows[kind][axis]
            place = data.at[pl.ds(0, data.shape[0] - 1)]
            remote(place, place, send, near.at[0], axis, places[axis][1]).wait_send()
        held, sems, send = bodies[kind][9:12]
        remote(held, held, send, sems.at[0], "row", row_others[0]).wait_send()


def store(src, dst, t, sem):
    half = src.shape[1] // 2
    for k in range(2):
        span = pl.ds(k * half, half)
        pltpu.make_async_copy(src.at[t, span], dst.at[t, span], sem).start(priority=k)


def scale_kernel(cols, lti, lto, r16i, r16o, fin, fout, ibase, obase, oin, oout, vib, vob, sems):
    slots = slots_of(cols)
    early = plans(vib.shape[0], vob.shape[0])[0][0][0][1]
    for t in range(early):
        store(vib, oin, t, sems.at[0])
    for number, (base, lt, r16, factor, out, begin) in enumerate(
        ((vib, lti, r16i, fin, oin, early), (vob, lto, r16o, fout, oout, 0))
    ):
        group = group_of(base.shape[0] - begin)

        @pl.loop(0, (base.shape[0] - begin) // group)
        def _(p):
            first = begin + p * group
            for u in range(group):
                scale_weight(base, lt, r16, factor, first + u, slots)
            for u in range(group):
                store(base, out, first + u, sems.at[number])

    pltpu.make_async_copy(vib, oin, sems.at[0]).wait()
    pltpu.make_async_copy(vob, oout, sems.at[1]).wait()


def pinned(arrays):
    return [pltpu.with_memory_space_constraint(a, pltpu.VMEM) for a in arrays]


def shards(rows, cols, inner_base, inner_left, inner_right, inner_mag, outer_base, outer_left, outer_right, outer_mag):
    rank = inner_left.shape[-1]
    ib = inner_base.reshape((-1, *inner_base.shape[-2:]))
    ob = outer_base.reshape((-1, *outer_base.shape[-2:]))
    il = jnp.swapaxes(inner_left, -1, -2).reshape((-1, rank, inner_left.shape[-2]))
    ol = jnp.swapaxes(outer_left, -1, -2).reshape((-1, rank, outer_left.shape[-2]))
    ir = inner_right.reshape((-1, *inner_right.shape[-2:]))
    orr = outer_right.reshape((-1, *outer_right.shape[-2:]))
    im = inner_mag.reshape((-1, *inner_mag.shape[-2:]))
    om = outer_mag.reshape((ob.shape[0], 1, -1))
    bf16, f32, dma = jnp.bfloat16, jnp.float32, pltpu.SemaphoreType.DMA
    bases = (ib, ob)
    work, cuts = plans(ib.shape[0], ob.shape[0])
    scratch = [pltpu.VMEM((n, *a.shape), bf16) for n, a in ((cols, il), (cols, ol), (rows, ir), (rows, orr))]
    for b, edges in zip(bases, work):
        scratch.append(pltpu.VMEM((max(end - begin for begin, end in edges), rank, b.shape[2]), f32))
    scratch.append(pltpu.VMEM((max(end - begin for begin, end in work[0]), 8, ib.shape[2]), f32))
    scratch += [pltpu.VMEM((b.shape[0], 1, b.shape[2]), f32) for b in bases]
    scratch += [pltpu.VMEM((rows - 1, b.shape[0], 1, b.shape[2]), f32) for b in bases]
    scratch += [pltpu.VMEM(m.shape, f32) for m in (im, om)]
    scratch += [dma((6,)), dma((6,))] + [dma((len(edges),)) for edges in work]
    for _ in range(2):
        for edges in cuts:
            scratch += [dma((len(edges),))] * 2
    scratch += [dma((len(edges),)) for edges in work]
    held = [pltpu.VMEM(b.shape, bf16) for b in bases]
    lefts = [pltpu.VMEM((b.shape[0], cols, b.shape[1] // cols, rank), bf16) for b in bases]
    rights = [pltpu.VMEM((b.shape[0], rank, b.shape[2]), bf16) for b in bases]
    factors = [pltpu.VMEM((b.shape[0], 1, b.shape[2]), f32) for b in bases]
    vib, vob, *rest = pinned(
        pl.pallas_call(
            functools.partial(collect_kernel, rows, cols),
            out_shape=held + lefts + rights + factors,
            in_specs=[ANY] * 8,
            out_specs=[VMEM] * 8,
            scratch_shapes=scratch,
            compiler_params=pltpu.CompilerParams(collective_id=0, has_side_effects=True, vmem_limit_bytes=GRANT),
            name="collect",
        )(il, ol, ir, orr, ib, ob, im, om)
    )
    inner, outer, _, _ = pl.pallas_call(
        functools.partial(scale_kernel, cols),
        out_shape=[jax.ShapeDtypeStruct(b.shape, bf16) for b in bases] + held,
        in_specs=[VMEM] * 8,
        out_specs=[ANY] * 2 + [VMEM] * 2,
        input_output_aliases={6: 2, 7: 3},
        scratch_shapes=[dma((2,))],
        compiler_params=pltpu.CompilerParams(vmem_limit_bytes=GRANT),
        name="scale",
    )(*rest, vib, vob)
    return inner.reshape(inner_base.shape), outer.reshape(outer_base.shape)


def solution(mesh):
    in_specs = (
        P(None, None, None, "row", "col"),
        P(None, None, None, ("row", "col"), None),
        P(None, None, None, "row", "col"),
        P(None, None, None, "col"),
        P(None, None, "row", "col"),
        P(None, None, ("row", "col"), None),
        P(None, None, "row", "col"),
        P(None, None, "col"),
    )
    out_specs = (P(None, None, None, "row", "col"), P(None, None, "row", "col"))
    body = functools.partial(shards, mesh.shape["row"], mesh.shape["col"])
    return jax.shard_map(body, mesh=mesh, in_specs=in_specs, out_specs=out_specs, check_vma=False)
```
